256 devices in a mesh: vocab: 64 (over z, y, core), layer: 4 (over x).
Axes of the slice: x: 4, y: 4, z: 8, core: 2. Of those that a mesh axis runs over, the one named last changes fastest.
Arguments:
- residual: bfloat16 [1024, 8192], P('layer', 'vocab'), may hold values from -40 to 40
- gain: bfloat16 [1, 8192], P(None, 'vocab'), may hold values from 0.25 to 1.75
- unembed: bfloat16 [8192, 128256], P(None, ('vocab', 'layer')), may hold values from -0.22097087 to 0.22097087
Outputs:
- log_probs: float32 [1024, 128256], P('layer', 'vocab')
The draws below stay inside these ranges and needn't reach their ends.
All inputs are finite; a program needn't handle non-finite values.
Results may differ from the reference program's by a relative error of at most 0.0003.
Values may be sent and summed in bfloat16 or wider, within the bound.
A program may use at most 128 MiB of HBM per device.

```python
import math
import jax
import jax.numpy as jnp
from jax import lax

D = 8192
VOCAB = 128256
TOK = 16
ROWS = 1024


def loud_offset(key):
    return jax.random.randint(jax.random.fold_in(key, 103), (), 0, 32)


def column_of(key, column):
    gaussian = jax.random.truncated_normal(jax.random.fold_in(jax.random.fold_in(key, 101), column), -4.0, 4.0, (D,), jnp.float32)
    spread = jax.random.uniform(jax.random.fold_in(jax.random.fold_in(key, 102), column), (), jnp.float32, -0.5, 0.5)
    loud = jnp.where(column % 32 == loud_offset(key), max(1.0, 80.0 / math.sqrt(D)), 1.0)
    return gaussian * (3.0 * jnp.exp(spread) * loud / math.sqrt(D))


def unit_column(key, column):
    vector = column_of(key, column)
    return vector / jnp.sqrt(jnp.mean(vector * vector))


def draw_unembed(key, part):
    columns = jax.vmap(lambda column: column_of(key, column))(jnp.arange(VOCAB))
    return columns.T.astype(jnp.bfloat16)


def draw_residual(key, part):
    offset = loud_offset(key)
    first = offset + 32 * jax.random.randint(jax.random.fold_in(key, 203), (ROWS,), 0, VOCAB // 32)
    second = offset + 32 * jax.random.randint(jax.random.fold_in(key, 204), (ROWS,), 0, VOCAB // 32)
    aligned = jax.vmap(lambda column: unit_column(key, column))(first)
    aligned = aligned + 0.99 * jax.vmap(lambda column: unit_column(key, column))(second)
    chosen = (jnp.arange(ROWS) % TOK == 0)[:, None]
    noise = jax.random.truncated_normal(jax.random.fold_in(key, 201), -4.0, 4.0, (ROWS, D), jnp.float32)
    scales = jnp.exp(jax.random.uniform(jax.random.fold_in(key, 202), (ROWS, 1), jnp.float32, 0.0, math.log(10.0)))
    strength = jnp.exp(jax.random.uniform(jax.random.fold_in(key, 205), (ROWS, 1), jnp.float32, math.log(0.2), math.log(2.0)))
    mixed = jnp.where(chosen, strength * (aligned + 0.1 * noise), noise * scales)
    return mixed.astype(jnp.bfloat16)


def setup_inputs(seed: int = 0) -> dict:
    key_of = jax.random.split(jax.random.key(seed), 4)
    residual = draw_residual(jax.random.fold_in(key_of[3], 71), 0)
    gain = jnp.clip(1.0 + 0.15 * jax.random.normal(key_of[1], (1, D), jnp.float32), 0.25, 1.75).astype(jnp.bfloat16)
    unembed = draw_unembed(jax.random.fold_in(key_of[3], 71), 0)
    return dict(residual=residual, gain=gain, unembed=unembed)


def reference(residual, gain, unembed):
    widened = residual.astype(jnp.float32)
    inverse = lax.rsqrt(lax.optimization_barrier(jnp.sum(widened * widened, axis=1)) / D + 1e-05)
    scaled = (widened * gain.astype(jnp.float32)).astype(jnp.bfloat16)
    logits = jnp.dot(scaled, unembed, preferred_element_type=jnp.float32) * inverse[:, None]
    highest = lax.optimization_barrier(jnp.max(logits, axis=1, keepdims=True))
    lse = highest + jnp.log(lax.optimization_barrier(jnp.sum(jnp.exp(logits - highest), axis=1, keepdims=True)))
    return logits - lse
```

```python
import jax
import jax.numpy as jnp
from jax import lax
from jax.experimental import pallas as pl
from jax.experimental.pallas import tpu as pltpu
from jax.sharding import Mesh
from jax.sharding import PartitionSpec as P

D = 8192
MESH = pl.DeviceIdType.MESH
AXES = ("z", "y", "c", "x")
NX, NZ, NY = 4, 8, 4
ROWS, FEAT, COLS = 256, 128, 501
WIDE = 512

HOPS = (
    641, 284, 388, 515, 160, 96, 3492, 3169, 3717, 3359, 3260, 3591,
    4376, 4707, 4220, 4765, 4488, 4257, 5312, 5762, 5220, 5667, 6537, 6247,
    6456, 6790, 6695, 6335, 7451, 7272, 7563, 7933, 7778, 7336, 8468, 8933,
    8319, 8588, 8771, 8412, 9766, 9881, 9643, 9524, 9284, 9405, 10639, 10345,
    10937, 10409, 10814, 10617, 11934, 11543, 11661, 11883, 11436, 11335, 12404, 12603,
    12491, 12949, 12744, 12826, 14010, 13584, 13715, 13528, 13838, 13423, 15029, 14509,
    14768, 14712, 14890, 14455, 15564, 16106, 15633, 15894, 15482, 15791, 16501, 16876,
    17097, 16752, 16563, 16951, 17901, 17613, 17718, 17518, 18058, 17938, 19121, 18931,
    19067, 18640, 18519, 18722, 19535, 20214, 20018, 19838, 19942, 19667, 20805, 20654,
    20978, 20593, 21198, 21029, 21972, 22225, 21855, 21589, 21722, 22107, 22742, 23114,
    23261, 22598, 23873, 24281, 23634, 24130, 23774,
)
LAG = 3
STEPS = ((1, 0, 0), (-1, 0, 0), (0, 1, 0), (0, -1, 0), (0, 0, 1), (0, 0, -1))


def plan():
    arrive = {0: 0}
    for hop in HOPS:
        arrive[hop % 128] = hop // 1024 + LAG
    last = max(arrive.values())
    rounds = []
    for r in range(last + 2):
        takes = [t for t in arrive if arrive[t] == r and t != 0]
        hops = [(hop // 128 % 8, hop % 128) for hop in HOPS if hop // 1024 == r]
        groups = [
            g for g in range(32) if max(arrive[g * 4 + k] for k in range(4)) + 1 == r
        ]
        rounds.append((takes, hops, groups))
    return rounds


def offset_of(t):
    return t // 32, t // 4 % 8, t % 4


def kernel(
    res_ref, gain_ref, unembed_ref, out_ref,
    held, weights, acc, logits, ssq_a, ssq_b, st_a, st_b,
    w_sem, hop_send, hop_recv, pair_send, pair_recv,
    blk_send, blk_recv, sq_send, sq_recv, st_send, st_recv,
):
    z, y, c, x = (lax.axis_index(a) for a in AXES)

    def at(dx, dz, dy, dc=0):
        return (
            lax.rem(z + dz % NZ, NZ), lax.rem(y + dy % NY, NY),
            lax.rem(c + dc, 2), lax.rem(x + dx % NX, NX),
        )

    def slot(dx, dz, dy):
        zz, yy, _, xx = at(dx, dz, dy)
        return (xx * NZ + zz) * NY + yy

    load = pltpu.make_async_copy(unembed_ref, weights, w_sem)
    load.start()

    widened = res_ref[...].astype(jnp.float32)
    mine = slot(0, 0, 0)
    held[c, mine] = (widened * gain_ref[...].astype(jnp.float32)).astype(jnp.bfloat16)
    squares = jnp.sum(jnp.transpose(widened * widened), axis=0, keepdims=True)
    ssq_a[0] = jnp.broadcast_to(squares, (8, ROWS))

    barrier = pltpu.get_barrier_semaphore()
    near = [at(*step) for step in STEPS] + [at(0, 0, 0, 1)]
    for device in near:
        pl.semaphore_signal(barrier, inc=1, device_id=device, device_id_type=MESH)
    pl.semaphore_wait(barrier, len(near))

    def send(src, dst, send_sem, recv_sem, device):
        copy = pltpu.make_async_remote_copy(
            src_ref=src, dst_ref=dst, send_sem=send_sem, recv_sem=recv_sem,
            device_id=device, device_id_type=MESH,
        )
        copy.start()
        return copy

    def pair_send_of(t):
        s = slot(*offset_of(t))
        send(held.at[c, s], held.at[c, s], pair_send.at[t], pair_recv.at[t], at(0, 0, 0, 1))

    def landed(ref, sem):
        pltpu.make_async_copy(ref, ref, sem).wait()

    def exchange(buf, send_sem, recv_sem, places):
        copies = [
            send(buf.at[0], buf.at[k + 1], send_sem.at[k], recv_sem.at[k], place)
            for k, place in enumerate(places)
        ]
        return copies

    plane = [at(0, 0, dy, dc) for dy in range(NY) for dc in range(2) if dy or dc]
    column = [at(0, dz, 0) for dz in range(1, NZ)]

    pair_send_of(0)
    acc[...] = jnp.zeros_like(acc)
    load.wait()

    def multiply(g):
        dx, dz = g // 8, g % 8
        xx, zz = lax.rem(x + dx, NX), lax.rem(z + dz, NZ)

        @pl.loop(0, NY)
        def _(dy):
            yy = lax.rem(y + dy, NY)
            s = (xx * NZ + zz) * NY + yy
            landed(held.at[1 - c, s], pair_recv.at[g * NY + dy])
            both = jnp.concatenate([held[0, s], held[1, s]], axis=1)
            start = pl.multiple_of((zz * NY + yy) * (2 * FEAT), 2 * FEAT)
            acc[xx] += jnp.dot(
                both, weights[pl.ds(start, 2 * FEAT), :], preferred_element_type=jnp.float32
            )

    done = {dx: 0 for dx in range(NX)}
    blocks = []
    columns_started = None
    planes_started = None
    for takes, hops, groups in plan():
        for t in takes:
            s = slot(*offset_of(t))
            landed(held.at[c, s], hop_recv.at[t])
            pair_send_of(t)
        for d, t in hops:
            dx, dz, dy = (a + b for a, b in zip(offset_of(t), STEPS[d]))
            s = slot(dx, dz, dy)
            send(held.at[c, s], held.at[c, s], hop_send.at[t], hop_recv.at[t], at(*STEPS[d]))
        for g in groups:
            multiply(g)
            if g == 0:
                planes_started = exchange(ssq_a, sq_send.at[0], sq_recv.at[0], plane)
            dx = g // 8
            done[dx] += 1
            if done[dx] == 8 and dx:
                xx = lax.rem(x + dx, NX)
                blocks.append(
                    send(acc.at[xx], logits.at[x], blk_send.at[dx - 1], blk_recv.at[dx - 1], at(dx, 0, 0))
                )

    for copy in planes_started:
        copy.wait()
    ssq_b[0] = jnp.sum(ssq_a[...], axis=0)
    for copy in exchange(ssq_b, sq_send.at[1], sq_recv.at[1], column):
        copy.wait()
    inverse = lax.rsqrt(jnp.sum(ssq_b[...], axis=0) / D + 1e-05)

    def to_column(lines):
        tall = jnp.concatenate([lines] * (FEAT // 8), axis=0)
        return jnp.transpose(tall)

    inverse_column = to_column(inverse)[:, :1]
    logits[x] = acc[x]
    for copy in blocks:
        copy.wait()

    lane = lax.broadcasted_iota(jnp.int32, (1, COLS), 1)
    del lane
    highest = jnp.full((ROWS, 1), -jnp.inf, jnp.float32)
    for k in range(NX):
        scaled = logits[k] * inverse_column
        logits[k] = scaled
        highest = jnp.maximum(highest, jnp.max(scaled, axis=1, keepdims=True))
    total = jnp.zeros((ROWS, 1), jnp.float32)
    for k in range(NX):
        total = total + jnp.sum(jnp.exp(logits[k] - highest), axis=1, keepdims=True)

    lanes = lax.broadcasted_iota(jnp.int32, (ROWS, FEAT), 1)
    packed = jnp.where(lanes == 0, highest, total)
    st_a[0] = jnp.transpose(packed)[:8]

    def merged(buf):
        top = buf[0][:1]
        for k in range(1, 8):
            top = jnp.maximum(top, buf[k][:1])
        add = jnp.zeros_like(top)
        for k in range(8):
            add = add + buf[k][1:2] * jnp.exp(buf[k][:1] - top)
        return top, add

    for copy in exchange(st_a, st_send.at[0], st_recv.at[0], plane):
        copy.wait()
    top, add = merged(st_a)
    line = lax.broadcasted_iota(jnp.int32, (8, ROWS), 0)
    st_b[0] = jnp.where(line == 0, top, add)
    for copy in exchange(st_b, st_send.at[1], st_recv.at[1], column):
        copy.wait()
    top, add = merged(st_b)
    lse = to_column(jnp.broadcast_to(top + jnp.log(add), (8, ROWS)))[:, :1]
    for k in range(NX):
        out_ref[:, COLS * k : COLS * (k + 1)] = logits[k] - lse

    @pl.loop(0, 128)
    def _(t):
        landed(held.at[c, t], pair_send.at[t])

    @pl.loop(1, 128)
    def _(t):
        landed(held.at[c, t], hop_send.at[t])


def local(residual, gain, unembed):
    f32, bf16 = jnp.float32, jnp.bfloat16
    vmem = pl.BlockSpec(memory_space=pltpu.VMEM)
    dma = pltpu.SemaphoreType.DMA
    return pl.pallas_call(
        kernel,
        name="lens",
        out_shape=jax.ShapeDtypeStruct((ROWS, NX * COLS), f32),
        in_specs=[vmem, vmem, pl.BlockSpec(memory_space=pl.ANY)],
        out_specs=vmem,
        scratch_shapes=[
            pltpu.VMEM((2, NX * NZ * NY, ROWS, FEAT), bf16),
            pltpu.VMEM((D, COLS), bf16),
            pltpu.VMEM((NX, ROWS, COLS), f32),
            pltpu.VMEM((NX, ROWS, COLS), f32),
            pltpu.VMEM((8, 8, ROWS), f32),
            pltpu.VMEM((8, 8, ROWS), f32),
            pltpu.VMEM((8, 8, ROWS), f32),
            pltpu.VMEM((8, 8, ROWS), f32),
            dma, dma((128,)), dma((128,)), dma((128,)), dma((128,)),
            dma((3,)), dma((3,)), dma((2, 7)), dma((2, 7)), dma((2, 7)), dma((2, 7)),
        ],
        compiler_params=pltpu.CompilerParams(
            collective_id=0, has_side_effects=True, vmem_limit_bytes=60 * 1024 * 1024
        ),
    )(residual, gain, unembed)


def solution(mesh):
    torus = Mesh(mesh.devices.reshape(NZ, NY, 2, mesh.shape["layer"]), AXES)
    planes = ("z", "y", "c")
    return jax.shard_map(
        local,
        mesh=torus,
        in_specs=(P("x", planes), P(None, planes), P(None, (*planes, "x"))),
        out_specs=P("x", planes),
        check_vma=False,
    )
```

```python
import jax
import jax.numpy as jnp
from jax import lax
from jax.experimental import pallas as pl
from jax.experimental.pallas import tpu as pltpu
from jax.sharding import Mesh
from jax.sharding import PartitionSpec as P

D = 8192
MESH = pl.DeviceIdType.MESH
AXES = ("z", "y", "c", "x")
NX, NZ, NY = 4, 8, 4
ROWS, FEAT, COLS = 256, 128, 501
SKIP = ()

HOPS = (
    641, 284, 388, 515, 160, 96, 3492, 3169, 3717, 3359, 3260, 3591,
    4376, 4707, 4220, 4765, 4488, 4257, 5312, 5762, 5220, 5667, 6537, 6247,
    6456, 6790, 6695, 6335, 7451, 7272, 7563, 7933, 7778, 7336, 8468, 8933,
    8319, 8588, 8771, 8412, 9766, 9881, 9643, 9524, 9284, 9405, 10639, 10345,
    10937, 10409, 10814, 10617, 11934, 11543, 11661, 11883, 11436, 11335, 12404, 12603,
    12491, 12949, 12744, 12826, 14010, 13584, 13715, 13528, 13838, 13423, 15029, 14509,
    14768, 14712, 14890, 14455, 15564, 16106, 15633, 15894, 15482, 15791, 16501, 16876,
    17097, 16752, 16563, 16951, 17901, 17613, 17718, 17518, 18058, 17938, 19121, 18931,
    19067, 18640, 18519, 18722, 19535, 20214, 20018, 19838, 19942, 19667, 20805, 20654,
    20978, 20593, 21198, 21029, 21972, 22225, 21855, 21589, 21722, 22107, 22742, 23114,
    23261, 22598, 23873, 24281, 23634, 24130, 23774,
)
LAG = 3
STEPS = ((1, 0, 0), (-1, 0, 0), (0, 1, 0), (0, -1, 0), (0, 0, 1), (0, 0, -1))


def plan():
    arrive = {0: 0}
    for hop in HOPS:
        arrive[hop % 128] = hop // 1024 + LAG
    last = max(arrive.values())
    rounds = []
    for r in range(last + 2):
        takes = [t for t in arrive if arrive[t] == r and t != 0]
        hops = [(hop // 128 % 8, hop % 128) for hop in HOPS if hop // 1024 == r]
        groups = [
            g for g in range(32) if max(arrive[g * 4 + k] for k in range(4)) + 1 == r
        ]
        rounds.append((takes, hops, groups))
    return rounds


def offset_of(t):
    return t // 32, t // 4 % 8, t % 4


def kernel(
    res_ref, gain_ref, unembed_ref, out_ref,
    held, weights, acc, logits, ssq_a, ssq_b, st_a, st_b,
    w_sem, hop_send, hop_recv, pair_send, pair_recv,
    blk_send, blk_recv, sq_send, sq_recv, st_send, st_recv,
):
    z, y, c, x = (lax.axis_index(a) for a in AXES)
    own_half = pl.ds(pl.multiple_of(c * FEAT, FEAT), FEAT)
    other_half = pl.ds(pl.multiple_of((1 - c) * FEAT, FEAT), FEAT)

    def at(dx, dz, dy, dc=0):
        return (
            lax.rem(z + dz % NZ, NZ), lax.rem(y + dy % NY, NY),
            lax.rem(c + dc, 2), lax.rem(x + dx % NX, NX),
        )

    def slot(dx, dz, dy):
        zz, yy, _, xx = at(dx, dz, dy)
        return (xx * NZ + zz) * NY + yy

    load = pltpu.make_async_copy(unembed_ref, weights, w_sem)
    load.start()

    widened = res_ref[...].astype(jnp.float32)
    scaled = (widened * gain_ref[...].astype(jnp.float32)).astype(jnp.bfloat16)
    held[slot(0, 0, 0), own_half] = jnp.transpose(scaled.astype(jnp.float32)).astype(jnp.bfloat16)
    squares = jnp.sum(jnp.transpose(widened * widened), axis=0, keepdims=True)
    ssq_a[0] = jnp.broadcast_to(squares, (8, ROWS))

    barrier = pltpu.get_barrier_semaphore()
    near = [at(*step) for step in STEPS] + [at(0, 0, 0, 1)]
    for device in near:
        pl.semaphore_signal(barrier, inc=1, device_id=device, device_id_type=MESH)
    pl.semaphore_wait(barrier, len(near))

    def send(src, dst, send_sem, recv_sem, device):
        copy = pltpu.make_async_remote_copy(
            src_ref=src, dst_ref=dst, send_sem=send_sem, recv_sem=recv_sem,
            device_id=device, device_id_type=MESH,
        )
        copy.start()
        return copy

    def pair_send_of(t):
        shard = held.at[slot(*offset_of(t)), own_half]
        send(shard, shard, pair_send.at[t], pair_recv.at[t], at(0, 0, 0, 1))

    def landed(ref, sem):
        pltpu.make_async_copy(ref, ref, sem).wait()

    def exchange(buf, send_sem, recv_sem, places):
        return [
            send(buf.at[0], buf.at[k + 1], send_sem.at[k], recv_sem.at[k], place)
            for k, place in enumerate(places)
        ]

    plane = [at(0, 0, dy, dc) for dy in range(NY) for dc in range(2) if dy or dc]
    column = [at(0, dz, 0) for dz in range(1, NZ)]

    if "pair" not in SKIP:
        pair_send_of(0)
    acc[...] = jnp.zeros_like(acc)

    def multiply(g):
        dx, dz = g // 8, g % 8
        xx, zz = lax.rem(x + dx, NX), lax.rem(z + dz, NZ)
        if "pair" not in SKIP:
            for dy in range(NY):
                landed(held.at[slot(dx, dz, dy), other_half], pair_recv.at[g * NY + dy])
        if "mm" in SKIP:
            return
        first = pl.multiple_of((xx * NZ + zz) * NY, NY)
        start = pl.multiple_of(zz * (2 * NY * FEAT), 2 * NY * FEAT)
        acc[xx] += jnp.dot(
            weights[:, pl.ds(start, 2 * NY * FEAT)],
            held[pl.ds(first, NY)].reshape(2 * NY * FEAT, ROWS),
            preferred_element_type=jnp.float32,
        )

    done = {dx: 0 for dx in range(NX)}
    blocks = []
    planes_started = None
    loaded = False
    for takes, hops, groups in plan():
        for t in takes:
            landed(held.at[slot(*offset_of(t)), own_half], hop_recv.at[t])
            if "pair" not in SKIP:
                pair_send_of(t)
        for d, t in hops:
            dx, dz, dy = (a + b for a, b in zip(offset_of(t), STEPS[d]))
            shard = held.at[slot(dx, dz, dy), own_half]
            send(shard, shard, hop_send.at[t], hop_recv.at[t], at(*STEPS[d]))
        for g in groups:
            if not loaded:
                load.wait()
                loaded = True
            multiply(g)
            if g == 0:
                planes_started = exchange(ssq_a, sq_send.at[0], sq_recv.at[0], plane)
            dx = g // 8
            done[dx] += 1
            if done[dx] == 8 and dx and "blk" not in SKIP:
                xx = lax.rem(x + dx, NX)
                blocks.append(
                    send(acc.at[xx], logits.at[x], blk_send.at[dx - 1], blk_recv.at[dx - 1], at(dx, 0, 0))
                )

    for copy in planes_started:
        copy.wait()
    ssq_b[0] = jnp.sum(ssq_a[...], axis=0)
    for copy in exchange(ssq_b, sq_send.at[1], sq_recv.at[1], column):
        copy.wait()
    inverse = lax.rsqrt(jnp.sum(ssq_b[...], axis=0)[:1] / D + 1e-05)

    logits[x] = acc[x]
    for copy in blocks:
        copy.wait()
    highest = jnp.full((1, ROWS), -jnp.inf, jnp.float32)
    for k in range(NX):
        highest = jnp.maximum(highest, jnp.max(logits[k] * inverse, axis=0, keepdims=True))
    total = jnp.zeros((1, ROWS), jnp.float32)
    for k in range(NX):
        total = total + jnp.sum(jnp.exp(logits[k] * inverse - highest), axis=0, keepdims=True)

    line = lax.broadcasted_iota(jnp.int32, (8, ROWS), 0)

    def merged(buf):
        top = buf[0][:1]
        for k in range(1, 8):
            top = jnp.maximum(top, buf[k][:1])
        add = jnp.zeros_like(top)
        for k in range(8):
            add = add + buf[k][1:2] * jnp.exp(buf[k][:1] - top)
        return top, add

    if "st" not in SKIP:
        st_a[0] = jnp.where(line == 0, highest, total)
        for copy in exchange(st_a, st_send.at[0], st_recv.at[0], plane):
            copy.wait()
        top, add = merged(st_a)
        st_b[0] = jnp.where(line == 0, top, add)
        for copy in exchange(st_b, st_send.at[1], st_recv.at[1], column):
            copy.wait()
        top, add = merged(st_b)
    else:
        top, add = highest, total
    lse = top + jnp.log(add)
    for k in range(NX):
        out_ref[COLS * k : COLS * (k + 1), :] = logits[k] * inverse - lse

    @pl.loop(0 if "pair" not in SKIP else 128, 128)
    def _(t):
        landed(held.at[t, own_half], pair_send.at[t])

    @pl.loop(1, 128)
    def _(t):
        landed(held.at[t, own_half], hop_send.at[t])


def local(residual, gain, unembed):
    f32, bf16 = jnp.float32, jnp.bfloat16
    vmem = pl.BlockSpec(memory_space=pltpu.VMEM)
    dma = pltpu.SemaphoreType.DMA
    out = pl.pallas_call(
        kernel,
        name="lens",
        out_shape=jax.ShapeDtypeStruct((NX * COLS, ROWS), f32),
        in_specs=[vmem, vmem, pl.BlockSpec(memory_space=pl.ANY)],
        out_specs=vmem,
        scratch_shapes=[
            pltpu.VMEM((NX * NZ * NY, 2 * FEAT, ROWS), bf16),
            pltpu.VMEM((COLS, D), bf16),
            pltpu.VMEM((NX, COLS, ROWS), f32),
            pltpu.VMEM((NX, COLS, ROWS), f32),
            pltpu.VMEM((8, 8, ROWS), f32),
            pltpu.VMEM((8, 8, ROWS), f32),
            pltpu.VMEM((8, 8, ROWS), f32),
            pltpu.VMEM((8, 8, ROWS), f32),
            dma, dma((128,)), dma((128,)), dma((128,)), dma((128,)),
            dma((3,)), dma((3,)), dma((2, 7)), dma((2, 7)), dma((2, 7)), dma((2, 7)),
        ],
        compiler_params=pltpu.CompilerParams(
            collective_id=0, has_side_effects=True, vmem_limit_bytes=60 * 1024 * 1024
        ),
    )(residual, gain, unembed.T)
    return out.T


def solution(mesh):
    torus = Mesh(mesh.devices.reshape(NZ, NY, 2, mesh.shape["layer"]), AXES)
    planes = ("z", "y", "c")
    return jax.shard_map(
        local,
        mesh=torus,
        in_specs=(P("x", planes), P(None, planes), P(None, (*planes, "x"))),
        out_specs=P("x", planes),
        check_vma=False,
    )
```

```python
import jax
import jax.numpy as jnp
from jax import lax
from jax.experimental import pallas as pl
from jax.experimental.pallas import tpu as pltpu
from jax.sharding import Mesh
from jax.sharding import PartitionSpec as P

D = 8192
MESH = pl.DeviceIdType.MESH
AXES = ("z", "y", "c", "x")
NX, NZ, NY = 4, 8, 4
ROWS, FEAT, COLS = 256, 128, 501

HOPS = (
    388, 284, 96, 515, 641, 160, 3619, 3809, 3236, 3452, 3172, 3463,
    4412, 4257, 4741, 4195, 4488, 4639, 5400, 5634, 5789, 5312, 6247, 6885,
    6311, 6783, 6568, 6520, 7743, 7480, 7333, 7842, 7272, 7563, 8802, 8893,
    8317, 8388, 8540, 8588, 9595, 9643, 9897, 9415, 9830, 9311, 10347, 10440,
    11001, 10732, 10612, 10811, 11692, 11838, 11480, 11357, 11572, 12009, 12966, 12717,
    12922, 12379, 12663, 12489, 13396, 13930, 13807, 13515, 14061, 13685, 14640, 14895,
    14540, 15029, 14832, 14406, 15565, 15731, 15793, 16046, 15927, 15450, 16471, 16881,
    17142, 16698, 17006, 16606, 17616, 17487, 17971, 17849, 18102, 17790, 19122, 18730,
    19058, 18517, 18641, 18832, 19795, 19534, 19601, 20185, 19914, 20054, 21189, 20756,
    20630, 21007, 20930, 20499, 22043, 21586, 21955, 21650, 21785, 22209, 22537, 23181,
    22814, 22933, 22679, 23050, 24078, 23962, 24198,
)
LAG = 3
STEPS = ((1, 0, 0), (-1, 0, 0), (0, 1, 0), (0, -1, 0), (0, 0, 1), (0, 0, -1))


SPAN = 86.5


def plan():
    arrive = {0: 0}
    for hop in HOPS:
        arrive[hop % 128] = hop // 1024 + LAG
    last = max(arrive.values())
    rounds = []
    for r in range(last + 2):
        takes = [t for t in arrive if arrive[t] == r and t != 0]
        hops = [(hop // 128 % 8, hop % 128) for hop in HOPS if hop // 1024 == r]
        groups = [
            g for g in range(32) if max(arrive[g * 4 + k] for k in range(4)) + 1 == r
        ]
        rounds.append((takes, hops, groups))
    x_last = max(hop // 1024 for hop in HOPS if hop // 128 % 8 < 2)
    came = {hop % 128: STEPS[hop // 128 % 8] for hop in HOPS}

    def moved(p, e, sign):
        return tuple((a + sign * b) % n for a, b, n in zip(p, e, (NX, NZ, NY)))

    known = {}
    for t in sorted(arrive, key=arrive.get):
        holder, p = (0, 0, 0), offset_of(t)
        shard = p
        while True:
            for near in (holder, *(moved(holder, e, 1) for e in STEPS)):
                known.setdefault(near, arrive[t])
            if holder == p:
                break
            e = came[(shard[0] * NZ + shard[1]) * NY + shard[2]]
            holder, shard = moved(holder, e, -1), moved(shard, e, 1)
    column_known = max(known[0, dz, 0] for dz in range(NZ))
    return rounds, x_last, column_known


def offset_of(t):
    return t // 32, t // 4 % 8, t % 4


def kernel(
    res_ref, gain_ref, unembed_ref, logits_ref, lse_ref,
    held, weights, acc, logits, code_out, code_in, note_out, note_in,
    ssq_a, ssq_b, ssq_c, st_a, st_b,
    w_sem, hop_send, hop_recv, pair_send, pair_recv,
    blk_send, blk_recv, note_send, note_recv, ex_send, ex_recv, out_sem,
):
    z, y, c, x = (lax.axis_index(a) for a in AXES)
    own_half = pl.ds(pl.multiple_of(c * FEAT, FEAT), FEAT)
    other_half = pl.ds(pl.multiple_of((1 - c) * FEAT, FEAT), FEAT)

    def at(dx, dz, dy, dc=0):
        return (
            lax.rem(z + dz % NZ, NZ), lax.rem(y + dy % NY, NY),
            lax.rem(c + dc, 2), lax.rem(x + dx % NX, NX),
        )

    def slot(dx, dz, dy):
        zz, yy, _, xx = at(dx, dz, dy)
        return (xx * NZ + zz) * NY + yy

    barrier = pltpu.get_barrier_semaphore()
    near = [at(*step) for step in STEPS] + [at(0, 0, 0, 1)]
    for device in near:
        pl.semaphore_signal(barrier, inc=1, device_id=device, device_id_type=MESH)
    load = pltpu.make_async_copy(unembed_ref, weights, w_sem)
    load.start()

    widened = res_ref[...].astype(jnp.float32)
    scaled = (widened * gain_ref[...].astype(jnp.float32)).astype(jnp.bfloat16)
    held[slot(0, 0, 0), own_half] = jnp.transpose(scaled.astype(jnp.float32)).astype(jnp.bfloat16)
    squares = jnp.sum(jnp.transpose(widened * widened), axis=0, keepdims=True)
    ssq_a[0] = jnp.broadcast_to(squares, (8, ROWS))
    acc[...] = jnp.zeros_like(acc)
    pl.semaphore_wait(barrier, len(near))

    def send(src, dst, send_sem, recv_sem, device):
        pltpu.make_async_remote_copy(
            src_ref=src, dst_ref=dst, send_sem=send_sem, recv_sem=recv_sem,
            device_id=device, device_id_type=MESH,
        ).start()

    def pair_send_of(t):
        shard = held.at[slot(*offset_of(t)), own_half]
        send(shard, shard, pair_send.at[t // 32], pair_recv.at[t // 4], at(0, 0, 0, 1))

    def landed(ref, sem):
        pltpu.make_async_copy(ref, ref, sem).wait()

    def exchange(buf, k, places):
        for n, place in enumerate(places):
            send(buf.at[0], buf.at[n + 1], ex_send.at[k], ex_recv.at[k], place)

    def exchanged(buf, k):
        rest = buf.at[pl.ds(1, buf.shape[0] - 1)]
        landed(rest, ex_recv.at[k])
        landed(rest, ex_send.at[k])

    plane = [at(0, 0, dy, dc) for dy in range(NY) for dc in range(2) if dy or dc]
    column = [at(0, dz, 0) for dz in range(1, NZ)]
    layers = [at(dx, 0, 0) for dx in range(1, NX)]

    def multiply(g):
        dx, dz = g // 8, g % 8
        xx, zz = lax.rem(x + dx, NX), lax.rem(z + dz, NZ)
        landed(held.at[pl.ds(0, NY), other_half], pair_recv.at[g])
        first = pl.multiple_of((xx * NZ + zz) * NY, NY)
        start = pl.multiple_of(zz * (2 * NY * FEAT), 2 * NY * FEAT)
        acc[xx] += jnp.dot(
            weights[:, pl.ds(start, 2 * NY * FEAT)],
            held[pl.ds(first, NY)].reshape(2 * NY * FEAT, ROWS),
            preferred_element_type=jnp.float32,
        )

    def inverse_of(dx):
        return lax.rsqrt(ssq_c[-dx % NX][:1] / D + 1e-05)

    def summed(values):
        highest = jnp.max(values, axis=0, keepdims=True)
        return highest, jnp.sum(jnp.exp(values - highest), axis=0, keepdims=True)

    def lines(*rows):
        line = lax.broadcasted_iota(jnp.int32, (8, ROWS), 0)
        out = jnp.broadcast_to(rows[-1], (8, ROWS))
        for k in range(len(rows) - 2, -1, -1):
            out = jnp.where(line == k, rows[k], out)
        return out

    def code_block(dx):
        values = acc[lax.rem(x + dx, NX)] * inverse_of(dx)
        highest, total = summed(values)
        reach = jnp.maximum(highest - jnp.min(values, axis=0, keepdims=True), 1e-20)
        note_out[dx - 1] = lines(highest, total, reach)
        send(note_out.at[dx - 1], note_in.at[dx - 1], note_send.at[dx - 1], note_recv.at[dx - 1], layers[dx - 1])
        step = 2 * SPAN / reach
        code_out[dx - 1] = jnp.exp(SPAN - (highest - values) * step).astype(jnp.bfloat16)

    def send_block(dx):
        send(code_out.at[dx - 1], code_in.at[dx - 1], blk_send.at[dx - 1], blk_recv.at[dx - 1], layers[dx - 1])

    pair_send_of(0)
    rounds, x_last, column_known = plan()
    whole = {dx: 0 for dx in range(NX)}
    loaded, squares_at = False, {}
    to_code, to_send = [], []
    for r, (takes, hops, groups) in enumerate(rounds):
        if takes:
            landed(held.at[pl.ds(0, len(takes)), own_half], hop_recv.at[r])
        for t in takes:
            pair_send_of(t)
        for d, t in hops:
            dx, dz, dy = (a + b for a, b in zip(offset_of(t), STEPS[d]))
            shard = held.at[slot(dx, dz, dy), own_half]
            send(shard, shard, hop_send.at[t // 32], hop_recv.at[r + LAG], at(*STEPS[d]))
        if r == squares_at.get("z"):
            exchanged(ssq_a, 0)
            ssq_b[0] = jnp.sum(ssq_a[...], axis=0)
            exchange(ssq_b, 1, column)
            squares_at["x"] = r + 4
        if r == squares_at.get("x"):
            exchanged(ssq_b, 1)
            ssq_c[0] = jnp.sum(ssq_b[...], axis=0)
            exchange(ssq_c, 2, layers)
            squares_at["done"] = r + 3
        if r == squares_at.get("done"):
            exchanged(ssq_c, 2)
        for g in groups:
            if not loaded:
                load.wait()
                loaded = True
            multiply(g)
            if g == 0:
                exchange(ssq_a, 0, plane)
                squares_at["z"] = max(r + 3, column_known)
            whole[g // 8] += 1
            if whole[g // 8] == 8 and g // 8:
                to_code.append(g // 8)
        if r >= squares_at.get("done", 1000):
            for dx in to_code:
                code_block(dx)
                to_send.append(dx)
            to_code = []
        if r >= x_last:
            for dx in to_send:
                send_block(dx)
            to_send = []
    assert not to_code and not to_send

    mine = acc[x] * inverse_of(0)
    tops, adds = [], []
    top, add = summed(mine)
    tops.append(top)
    adds.append(add)
    for k in range(NX - 1):
        landed(note_in.at[k], note_recv.at[k])
        tops.append(note_in[k][:1])
        adds.append(note_in[k][1:2])

    def merged(tops, adds):
        top = tops[0]
        for other in tops[1:]:
            top = jnp.maximum(top, other)
        add = jnp.zeros_like(top)
        for k in range(len(tops)):
            add = add + adds[k] * jnp.exp(tops[k] - top)
        return top, add

    st_a[0] = lines(*merged(tops, adds))
    exchange(st_a, 3, plane)
    logits[x] = mine
    exchanged(st_a, 3)
    st_b[0] = lines(*merged([st_a[k][:1] for k in range(8)], [st_a[k][1:2] for k in range(8)]))
    exchange(st_b, 4, column)

    for dx in (1, 3, 2):
        landed(code_in.at[dx - 1], blk_recv.at[dx - 1])
        note = note_in[dx - 1]
        highest, reach = note[:1], note[2:3]
        step = reach / (2 * SPAN)
        logits[lax.rem(x + NX - dx, NX)] = highest - (SPAN - jnp.log(code_in[dx - 1].astype(jnp.float32))) * step
    put = pltpu.make_async_copy(logits, logits_ref, out_sem)
    put.start()

    for dx in range(NX):
        landed(held.at[pl.ds(0, 32), own_half], pair_send.at[dx])
        landed(held.at[pl.ds(0, 31 if dx == 0 else 32), own_half], hop_send.at[dx])
    for k in range(NX - 1):
        landed(note_out.at[k], note_send.at[k])
        landed(code_out.at[k], blk_send.at[k])

    exchanged(st_b, 4)
    top, add = merged([st_b[k][:1] for k in range(8)], [st_b[k][1:2] for k in range(8)])
    lse_ref[...] = jnp.broadcast_to(top + jnp.log(add), (8, ROWS))
    put.wait()


def subtract(logits_ref, lse_ref, out_ref):
    lse = lse_ref[:1]
    for k in range(NX):
        out_ref[COLS * k : COLS * (k + 1), :] = logits_ref[k] - lse


def local(residual, gain, unembed):
    f32, bf16 = jnp.float32, jnp.bfloat16
    vmem = pl.BlockSpec(memory_space=pltpu.VMEM)
    anywhere = pl.BlockSpec(memory_space=pl.ANY)
    dma = pltpu.SemaphoreType.DMA
    logits, lse = pl.pallas_call(
        kernel,
        name="lens",
        out_shape=(
            jax.ShapeDtypeStruct((NX, COLS, ROWS), f32),
            jax.ShapeDtypeStruct((8, ROWS), f32),
        ),
        in_specs=[vmem, vmem, anywhere],
        out_specs=(anywhere, vmem),
        scratch_shapes=[
            pltpu.VMEM((NX * NZ * NY, 2 * FEAT, ROWS), bf16),
            pltpu.VMEM((COLS, D), bf16),
            pltpu.VMEM((NX, COLS, ROWS), f32),
            pltpu.VMEM((NX, COLS, ROWS), f32),
            pltpu.VMEM((NX - 1, COLS, ROWS), bf16),
            pltpu.VMEM((NX - 1, COLS, ROWS), bf16),
            pltpu.VMEM((NX - 1, 8, ROWS), f32),
            pltpu.VMEM((NX - 1, 8, ROWS), f32),
            pltpu.VMEM((8, 8, ROWS), f32),
            pltpu.VMEM((8, 8, ROWS), f32),
            pltpu.VMEM((NX, 8, ROWS), f32),
            pltpu.VMEM((8, 8, ROWS), f32),
            pltpu.VMEM((8, 8, ROWS), f32),
            dma, dma((4,)), dma((len(plan()[0]),)), dma((4,)), dma((32,)),
            dma((3,)), dma((3,)), dma((3,)), dma((3,)), dma((5,)), dma((5,)), dma,
        ],
        compiler_params=pltpu.CompilerParams(
            collective_id=0, has_side_effects=True, vmem_limit_bytes=58 * 1024 * 1024
        ),
    )(residual, gain, unembed.T)
    out = pl.pallas_call(
        subtract,
        name="subtract",
        out_shape=jax.ShapeDtypeStruct((NX * COLS, ROWS), f32),
        in_specs=[vmem, vmem],
        out_specs=vmem,
        compiler_params=pltpu.CompilerParams(vmem_limit_bytes=8 * 1024 * 1024),
    )(logits, lse)
    return out.T


def solution(mesh):
    torus = Mesh(mesh.devices.reshape(NZ, NY, 2, mesh.shape["layer"]), AXES)
    planes = ("z", "y", "c")
    return jax.shard_map(
        local,
        mesh=torus,
        in_specs=(P("x", planes), P(None, planes), P(None, (*planes, "x"))),
        out_specs=P("x", planes),
        check_vma=False,
    )
```

```python
import jax
import jax.numpy as jnp
from jax import lax
from jax.experimental import pallas as pl
from jax.experimental.pallas import tpu as pltpu
from jax.sharding import Mesh
from jax.sharding import PartitionSpec as P

D = 8192
MESH = pl.DeviceIdType.MESH
AXES = ("z", "y", "c", "x")
NX, NZ, NY = 4, 8, 4
ROWS, FEAT, COLS = 256, 128, 501

HOPS = (
    132376, 132488, 65820, 65632, 65696, 65924, 66177, 66051, 69155, 68769, 69345, 68988,
    68707, 69028, 69732, 69948, 70274, 70175, 69824, 70023, 71052, 71305, 70824, 71195,
    70760, 70932, 71800, 71999, 71864, 72418, 72167, 72226, 73085, 73445, 72831, 73255,
    72899, 73125, 73897, 74156, 74283, 74045, 74473, 73851, 75174, 75070, 75449, 75371,
    74939, 74868, 76518, 76268, 75956, 76414, 76153, 75842, 77175, 77293, 77485, 77003,
    77354, 76869, 77915, 78319, 78138, 78458, 78570, 78022, 79279, 79152, 78943, 79415,
    79605, 79070, 79949, 80369, 80243, 80558, 80074, 80502, 81646, 80975, 81329, 81498,
    81097, 81206, 82416, 82229, 82135, 82005, 82483, 82631, 83698, 83378, 83027, 83532,
    83150, 83292, 84433, 84673, 84054, 84185, 84247, 84573, 85200, 85716, 85278, 85444,
    85576, 85080, 86677, 86482, 86543, 86158, 86288, 86038, 87186, 87046, 87578, 87315,
    87435, 87690, 88349, 88717, 88453, 89361, 89497,
)
LAG = 3
STEPS = ((1, 0, 0), (-1, 0, 0), (0, 1, 0), (0, -1, 0), (0, 0, 1), (0, 0, -1))


SPAN = 86.5
SPLIT = 304


def parts_of(hop):
    links, r, d, t = hop // 65536, hop // 1024 % 64, hop // 128 % 8, hop % 128
    return links, r, d, t, tuple(links * a for a in STEPS[d])


def plan():
    arrive = {0: 0}
    for hop in HOPS:
        links, r, _, t, _ = parts_of(hop)
        arrive[t] = r + links - 1 + LAG
    last = max(arrive.values())
    rounds = []
    for r in range(last + 2):
        takes = [t for t in arrive if arrive[t] == r]
        hops = [(parts_of(hop)[4], hop % 128, arrive[hop % 128]) for hop in HOPS if parts_of(hop)[1] == r]
        rounds.append((takes, hops))
    x_last = max(parts_of(hop)[1] for hop in HOPS if parts_of(hop)[2] < 2)
    came = {hop % 128: parts_of(hop)[4] for hop in HOPS}

    def moved(p, e, sign):
        return tuple((a + sign * b) % n for a, b, n in zip(p, e, (NX, NZ, NY)))

    known, passed = {}, {}
    for t in sorted(arrive, key=arrive.get):
        holder, p = (0, 0, 0), offset_of(t)
        shard = p
        while True:
            passed.setdefault(holder, arrive[t])
            for near in (holder, *(moved(holder, e, 1) for e in STEPS)):
                known.setdefault(near, arrive[t])
            if holder == p:
                break
            e = came[(shard[0] * NZ + shard[1]) * NY + shard[2]]
            holder, shard = moved(holder, e, -1), moved(shard, e, 1)
    column_known = max(known[0, dz, 0] for dz in range(NZ))
    plane_known = max(passed[0, 0, dy] for dy in range(NY))
    return rounds, x_last, plane_known, column_known


def offset_of(t):
    return t // 32, t // 4 % 8, t % 4


def kernel(
    res_ref, gain_ref, unembed_ref, logits_ref, lse_ref,
    held, weights, acc, logits, code_out, code_in, passed, note_out, note_in,
    ssq_a, ssq_b, ssq_c, st_a, st_b,
    w_sem, hop_send, hop_recv, pair_send, pair_recv,
    blk_send, blk_recv, note_send, note_recv, ex_send, ex_recv, out_sem,
):
    z, y, c, x = (lax.axis_index(a) for a in AXES)
    own_half = pl.ds(pl.multiple_of(c * FEAT, FEAT), FEAT)
    other_half = pl.ds(pl.multiple_of((1 - c) * FEAT, FEAT), FEAT)

    def at(dx, dz, dy, dc=0):
        return (
            lax.rem(z + dz % NZ, NZ), lax.rem(y + dy % NY, NY),
            lax.rem(c + dc, 2), lax.rem(x + dx % NX, NX),
        )

    def slot(dx, dz, dy):
        zz, yy, _, xx = at(dx, dz, dy)
        return (xx * NZ + zz) * NY + yy

    barrier = pltpu.get_barrier_semaphore()
    near = [at(*step) for step in STEPS] + [at(0, 0, 0, 1), at(0, 2, 0), at(0, -2, 0)]
    for device in near:
        pl.semaphore_signal(barrier, inc=1, device_id=device, device_id_type=MESH)
    load = pltpu.make_async_copy(unembed_ref, weights, w_sem)
    load.start()

    widened = res_ref[...].astype(jnp.float32)
    scaled = (widened * gain_ref[...].astype(jnp.float32)).astype(jnp.bfloat16)
    held[slot(0, 0, 0), own_half] = jnp.transpose(scaled.astype(jnp.float32)).astype(jnp.bfloat16)
    squares = jnp.sum(jnp.transpose(widened * widened), axis=0, keepdims=True)
    ssq_a[0] = squares
    acc[...] = jnp.zeros_like(acc)
    pl.semaphore_wait(barrier, len(near))

    def send(src, dst, send_sem, recv_sem, device):
        pltpu.make_async_remote_copy(
            src_ref=src, dst_ref=dst, send_sem=send_sem, recv_sem=recv_sem,
            device_id=device, device_id_type=MESH,
        ).start()

    def pair_send_of(t, r):
        shard = held.at[slot(*offset_of(t)), own_half]
        send(shard, shard, pair_send.at[t // 32], pair_recv.at[r], at(0, 0, 0, 1))

    def landed(ref, sem):
        pltpu.make_async_copy(ref, ref, sem).wait()

    def exchange(buf, k, places):
        for n, place in enumerate(places):
            send(buf.at[0], buf.at[n + 1], ex_send.at[k], ex_recv.at[k], place)

    def exchanged(buf, k):
        rest = buf.at[pl.ds(1, buf.shape[0] - 1)]
        landed(rest, ex_recv.at[k])
        landed(rest, ex_send.at[k])

    plane = [at(0, 0, dy, dc) for dy in range(NY) for dc in range(2) if dy or dc]
    column = [at(0, dz, 0) for dz in range(1, NZ)]
    layers = [at(dx, 0, 0) for dx in range(1, NX)]

    def multiply(shards, r):
        landed(held.at[pl.ds(0, len(shards)), other_half], pair_recv.at[r])

        @pl.loop(0, len(shards))
        def _(n):
            t = shards[0]
            for k in range(1, len(shards)):
                t = jnp.where(n == k, shards[k], t)
            xx, zz = lax.rem(x + t // 32, NX), lax.rem(z + t // 4 % NZ, NZ)
            yy = lax.rem(y + t % NY, NY)
            start = pl.multiple_of((zz * NY + yy) * (2 * FEAT), 2 * FEAT)
            acc[xx] += jnp.dot(
                weights[:, pl.ds(start, 2 * FEAT)],
                held[(xx * NZ + zz) * NY + yy],
                preferred_element_type=jnp.float32,
            )

    def inverse_of(dx):
        return lax.rsqrt(ssq_c[-dx % NX] / D + 1e-05)

    def summed(values):
        highest = jnp.max(values, axis=0, keepdims=True)
        return highest, jnp.sum(jnp.exp(values - highest), axis=0, keepdims=True)

    def lines(*rows):
        count = 2 if len(rows) == 2 else 4
        line = lax.broadcasted_iota(jnp.int32, (count, ROWS), 0)
        out = jnp.broadcast_to(rows[-1], (count, ROWS))
        for k in range(len(rows) - 2, -1, -1):
            out = jnp.where(line == k, rows[k], out)
        return out

    def code_block(dx):
        values = acc[lax.rem(x + dx, NX)] * inverse_of(dx)
        highest, total = summed(values)
        reach = jnp.maximum(highest - jnp.min(values, axis=0, keepdims=True), 1e-20)
        note_out[dx - 1] = lines(highest, total, reach)
        send(note_out.at[dx - 1], note_in.at[dx - 1], note_send.at[dx - 1], note_recv.at[dx - 1], layers[dx - 1])
        step = 2 * SPAN / reach
        code_out[dx - 1] = jnp.exp(SPAN - (highest - values) * step).astype(jnp.bfloat16)

    near_part, far_part = pl.ds(0, SPLIT), pl.ds(SPLIT, COLS - SPLIT)

    def send_block(dx):
        if dx == 2:
            send(code_out.at[1, far_part], passed, blk_send.at[3], blk_recv.at[3], at(-1, 0, 0))
            send(code_out.at[1, near_part], code_in.at[1, near_part], blk_send.at[1], blk_recv.at[1], at(2, 0, 0))
        else:
            send(code_out.at[dx - 1], code_in.at[dx - 1], blk_send.at[dx - 1], blk_recv.at[dx - 1], layers[dx - 1])

    pair_send_of(0, 0)
    rounds, x_last, plane_known, column_known = plan()
    left = {dx: 32 for dx in range(NX)}
    squares_at = {}
    to_code, to_send, ready = [], [], ()
    for r, (takes, hops) in enumerate(rounds):
        if takes and r:
            landed(held.at[pl.ds(0, len(takes)), own_half], hop_recv.at[r])
            for t in takes:
                pair_send_of(t, r)
        for way, t, lands in hops:
            shard = held.at[slot(*(a + b for a, b in zip(offset_of(t), way))), own_half]
            send(shard, shard, hop_send.at[t // 32], hop_recv.at[lands], at(*way))
        if r == squares_at.get("z"):
            exchanged(ssq_a, 0)
            ssq_b[0] = jnp.sum(ssq_a[...], axis=0)
            exchange(ssq_b, 1, column)
            squares_at["x"] = r + 5
        if r == squares_at.get("x"):
            exchanged(ssq_b, 1)
            ssq_c[0] = jnp.sum(ssq_b[...], axis=0)
            exchange(ssq_c, 2, layers)
            squares_at["done"] = r + 4
        if r == squares_at.get("done"):
            exchanged(ssq_c, 2)
        if r == 1:
            load.wait()
        if ready:
            multiply(ready, r - 1)
        for t in ready:
            left[t // 32] -= 1
            if left[t // 32] == 0 and t // 32:
                to_code.append(t // 32)
        ready = takes
        if r == plane_known:
            exchange(ssq_a, 0, plane)
            squares_at["z"] = max(r + 4, column_known)
        if r >= squares_at.get("done", 1000):
            for dx in to_code:
                code_block(dx)
                to_send.append(dx)
            to_code = []
        if r >= x_last:
            for dx in to_send:
                send_block(dx)
            to_send = []
    assert not to_code and not to_send

    mine = acc[x] * inverse_of(0)
    tops, adds = [], []
    top, add = summed(mine)
    tops.append(top)
    adds.append(add)
    for k in range(NX - 1):
        landed(note_in.at[k], note_recv.at[k])
        tops.append(note_in[k][:1])
        adds.append(note_in[k][1:2])

    def merged(tops, adds):
        top = tops[0]
        for other in tops[1:]:
            top = jnp.maximum(top, other)
        add = jnp.zeros_like(top)
        for k in range(len(tops)):
            add = add + adds[k] * jnp.exp(tops[k] - top)
        return top, add

    st_a[0] = lines(*merged(tops, adds))
    exchange(st_a, 3, plane)
    landed(passed, blk_recv.at[3])
    send(passed, code_in.at[1, far_part], blk_send.at[4], blk_recv.at[4], at(-1, 0, 0))
    logits[x] = mine
    exchanged(st_a, 3)
    st_b[0] = lines(*merged([st_a[k][:1] for k in range(8)], [st_a[k][1:2] for k in range(8)]))
    exchange(st_b, 4, column)

    for dx in (1, 3, 2):
        if dx == 2:
            landed(code_in.at[1, near_part], blk_recv.at[1])
            landed(code_in.at[1, far_part], blk_recv.at[4])
        else:
            landed(code_in.at[dx - 1], blk_recv.at[dx - 1])
        note = note_in[dx - 1]
        highest, reach = note[:1], note[2:3]
        step = reach / (2 * SPAN)
        logits[lax.rem(x + NX - dx, NX)] = highest - (SPAN - jnp.log(code_in[dx - 1].astype(jnp.float32))) * step
    put = pltpu.make_async_copy(logits, logits_ref, out_sem)
    put.start()

    for dx in range(NX):
        landed(held.at[pl.ds(0, 32), own_half], pair_send.at[dx])
        landed(held.at[pl.ds(0, 31 if dx == 0 else 32), own_half], hop_send.at[dx])
    for k in range(NX - 1):
        landed(note_out.at[k], note_send.at[k])
        if k != 1:
            landed(code_out.at[k], blk_send.at[k])
    landed(code_out.at[1, near_part], blk_send.at[1])
    landed(passed, blk_send.at[3])
    landed(passed, blk_send.at[4])

    exchanged(st_b, 4)
    top, add = merged([st_b[k][:1] for k in range(8)], [st_b[k][1:2] for k in range(8)])
    lse_ref[...] = jnp.broadcast_to(top + jnp.log(add), (8, ROWS))
    put.wait()


def subtract(logits_ref, lse_ref, out_ref):
    lse = lse_ref[:1]
    for k in range(NX):
        out_ref[COLS * k : COLS * (k + 1), :] = logits_ref[k] - lse


def local(residual, gain, unembed):
    f32, bf16 = jnp.float32, jnp.bfloat16
    vmem = pl.BlockSpec(memory_space=pltpu.VMEM)
    anywhere = pl.BlockSpec(memory_space=pl.ANY)
    dma = pltpu.SemaphoreType.DMA
    logits, lse = pl.pallas_call(
        kernel,
        name="lens",
        out_shape=(
            jax.ShapeDtypeStruct((NX, COLS, ROWS), f32),
            jax.ShapeDtypeStruct((8, ROWS), f32),
        ),
        in_specs=[vmem, vmem, anywhere],
        out_specs=(anywhere, vmem),
        scratch_shapes=[
            pltpu.VMEM((NX * NZ * NY, 2 * FEAT, ROWS), bf16),
            pltpu.VMEM((COLS, D), bf16),
            pltpu.VMEM((NX, COLS, ROWS), f32),
            pltpu.VMEM((NX, COLS, ROWS), f32),
            pltpu.VMEM((NX - 1, COLS, ROWS), bf16),
            pltpu.VMEM((NX - 1, COLS, ROWS), bf16),
            pltpu.VMEM((COLS - SPLIT, ROWS), bf16),
            pltpu.VMEM((NX - 1, 4, ROWS), f32),
            pltpu.VMEM((NX - 1, 4, ROWS), f32),
            pltpu.VMEM((8, 1, ROWS), f32),
            pltpu.VMEM((8, 1, ROWS), f32),
            pltpu.VMEM((NX, 1, ROWS), f32),
            pltpu.VMEM((8, 2, ROWS), f32),
            pltpu.VMEM((8, 2, ROWS), f32),
            dma, dma((4,)), dma((len(plan()[0]),)), dma((4,)), dma((len(plan()[0]),)),
            dma((5,)), dma((5,)), dma((3,)), dma((3,)), dma((5,)), dma((5,)), dma,
        ],
        compiler_params=pltpu.CompilerParams(
            collective_id=0, has_side_effects=True, vmem_limit_bytes=50 * 1024 * 1024
        ),
    )(residual, gain, unembed.T)
    out = pl.pallas_call(
        subtract,
        name="subtract",
        out_shape=jax.ShapeDtypeStruct((NX * COLS, ROWS), f32),
        in_specs=[vmem, vmem],
        out_specs=vmem,
        compiler_params=pltpu.CompilerParams(vmem_limit_bytes=8 * 1024 * 1024),
    )(logits, lse)
    return out.T


def solution(mesh):
    torus = Mesh(mesh.devices.reshape(NZ, NY, 2, mesh.shape["layer"]), AXES)
    planes = ("z", "y", "c")
    return jax.shard_map(
        local,
        mesh=torus,
        in_specs=(P("x", planes), P(None, planes), P(None, (*planes, "x"))),
        out_specs=P("x", planes),
        check_vma=False,
    )
```

```python
import jax
import jax.numpy as jnp
from jax import lax
from jax.experimental import pallas as pl
from jax.experimental.pallas import tpu as pltpu
from jax.sharding import Mesh
from jax.sharding import PartitionSpec as P

D = 8192
MESH = pl.DeviceIdType.MESH
AXES = ("z", "y", "c", "x")
NX, NZ, NY = 4, 8, 4
ROWS, FEAT, COLS = 256, 128, 501

HOPS = (
    132376, 132488, 65820, 65632, 65696, 65924, 66177, 66051, 69155, 68769, 69345, 68988,
    68707, 69028, 69732, 69948, 70274, 70175, 69824, 70023, 71052, 71305, 70824, 71195,
    70760, 70932, 71800, 71999, 71864, 72418, 72167, 72226, 73085, 73445, 72831, 73255,
    72899, 73125, 73897, 74156, 74283, 74045, 74473, 73851, 75174, 75070, 75449, 75371,
    74939, 74868, 76518, 76268, 75956, 76414, 76153, 75842, 77175, 77293, 77485, 77003,
    77354, 76869, 77915, 78319, 78138, 78458, 78570, 78022, 79279, 79152, 78943, 79415,
    79605, 79070, 79949, 80369, 80243, 80558, 80074, 80502, 81646, 80975, 81329, 81498,
    81097, 81206, 82416, 82229, 82135, 82005, 82483, 82631, 83698, 83378, 83027, 83532,
    83150, 83292, 84433, 84673, 84054, 84185, 84247, 84573, 85200, 85716, 85278, 85444,
    85576, 85080, 86677, 86482, 86543, 86158, 86288, 86038, 87186, 87046, 87578, 87315,
    87435, 87690, 88349, 88717, 88453, 89361, 89497,
)
LAG = 3
STEPS = ((1, 0, 0), (-1, 0, 0), (0, 1, 0), (0, -1, 0), (0, 0, 1), (0, 0, -1))


SPAN = 86.5
SPLIT = 304


def parts_of(hop):
    links, r, d, t = hop // 65536, hop // 1024 % 64, hop // 128 % 8, hop % 128
    return links, r, d, t, tuple(links * a for a in STEPS[d])


def plan():
    arrive = {0: 0}
    for hop in HOPS:
        links, r, _, t, _ = parts_of(hop)
        arrive[t] = r + links - 1 + LAG
    last = max(arrive.values())
    rounds = []
    for r in range(last + 2):
        takes = [t for t in arrive if arrive[t] == r]
        hops = [(parts_of(hop)[4], hop % 128, arrive[hop % 128]) for hop in HOPS if parts_of(hop)[1] == r]
        rounds.append((takes, hops))
    x_last = max(parts_of(hop)[1] for hop in HOPS if parts_of(hop)[2] < 2)
    came = {hop % 128: parts_of(hop)[4] for hop in HOPS}

    def moved(p, e, sign):
        return tuple((a + sign * b) % n for a, b, n in zip(p, e, (NX, NZ, NY)))

    known, passed = {}, {}
    for t in sorted(arrive, key=arrive.get):
        holder, p = (0, 0, 0), offset_of(t)
        shard = p
        while True:
            passed.setdefault(holder, arrive[t])
            for near in (holder, *(moved(holder, e, 1) for e in STEPS)):
                known.setdefault(near, arrive[t])
            if holder == p:
                break
            e = came[(shard[0] * NZ + shard[1]) * NY + shard[2]]
            holder, shard = moved(holder, e, -1), moved(shard, e, 1)
    column_known = max(known[0, dz, 0] for dz in range(NZ))
    plane_known = max(passed[0, 0, dy] for dy in range(NY))
    return rounds, x_last, plane_known, column_known


def offset_of(t):
    return t // 32, t // 4 % 8, t % 4


def kernel(
    res_ref, gain_ref, unembed_ref, logits_ref, lse_ref,
    res, gain, held, weights, acc, code_out, code_in, passed, note_out, note_in,
    ssq_a, ssq_b, ssq_c, st_a, st_b,
    w_sem, hop_send, hop_recv, pair_send, pair_recv,
    blk_send, blk_recv, note_send, note_recv, ex_send, ex_recv, out_sem, in_sem,
):
    z, y, c, x = (lax.axis_index(a) for a in AXES)
    own_half = pl.ds(pl.multiple_of(c * FEAT, FEAT), FEAT)
    other_half = pl.ds(pl.multiple_of((1 - c) * FEAT, FEAT), FEAT)

    def at(dx, dz, dy, dc=0):
        return (
            lax.rem(z + dz % NZ, NZ), lax.rem(y + dy % NY, NY),
            lax.rem(c + dc, 2), lax.rem(x + dx % NX, NX),
        )

    def slot(dx, dz, dy):
        zz, yy, _, xx = at(dx, dz, dy)
        return (xx * NZ + zz) * NY + yy

    barrier = pltpu.get_barrier_semaphore()
    near = [at(*step) for step in STEPS] + [at(0, 0, 0, 1), at(0, 2, 0), at(0, -2, 0)]
    for device in near:
        pl.semaphore_signal(barrier, inc=1, device_id=device, device_id_type=MESH)
    brought = [
        pltpu.make_async_copy(res_ref, res, in_sem.at[0]),
        pltpu.make_async_copy(gain_ref, gain, in_sem.at[1]),
    ]
    load = pltpu.make_async_copy(unembed_ref, weights, w_sem)
    for copy in (*brought, load):
        copy.start()

    for copy in brought:
        copy.wait()
    widened = res[...].astype(jnp.float32)
    scaled = (widened * gain[...].astype(jnp.float32)).astype(jnp.bfloat16)
    held[slot(0, 0, 0), own_half] = jnp.transpose(scaled.astype(jnp.float32)).astype(jnp.bfloat16)
    squares = jnp.sum(jnp.transpose(widened * widened), axis=0, keepdims=True)
    ssq_a[0] = squares
    acc[...] = jnp.zeros_like(acc)
    pl.semaphore_wait(barrier, len(near))

    def send(src, dst, send_sem, recv_sem, device):
        pltpu.make_async_remote_copy(
            src_ref=src, dst_ref=dst, send_sem=send_sem, recv_sem=recv_sem,
            device_id=device, device_id_type=MESH,
        ).start()

    def pair_send_of(t, r):
        shard = held.at[slot(*offset_of(t)), own_half]
        send(shard, shard, pair_send.at[t // 32], pair_recv.at[r], at(0, 0, 0, 1))

    def landed(ref, sem):
        pltpu.make_async_copy(ref, ref, sem).wait()

    def exchange(buf, k, places):
        for n, place in enumerate(places):
            send(buf.at[0], buf.at[n + 1], ex_send.at[k], ex_recv.at[k], place)

    def exchanged(buf, k):
        rest = buf.at[pl.ds(1, buf.shape[0] - 1)]
        landed(rest, ex_recv.at[k])
        landed(rest, ex_send.at[k])

    plane = [at(0, 0, dy, dc) for dy in range(NY) for dc in range(2) if dy or dc]
    column = [at(0, dz, 0) for dz in range(1, NZ)]
    layers = [at(dx, 0, 0) for dx in range(1, NX)]

    def multiply(shards, r):
        landed(held.at[pl.ds(0, len(shards)), other_half], pair_recv.at[r])

        @pl.loop(0, len(shards))
        def _(n):
            t = shards[0]
            for k in range(1, len(shards)):
                t = jnp.where(n == k, shards[k], t)
            xx, zz = lax.rem(x + t // 32, NX), lax.rem(z + t // 4 % NZ, NZ)
            yy = lax.rem(y + t % NY, NY)
            start = pl.multiple_of((zz * NY + yy) * (2 * FEAT), 2 * FEAT)
            acc[xx] += jnp.dot(
                weights[:, pl.ds(start, 2 * FEAT)],
                held[(xx * NZ + zz) * NY + yy],
                preferred_element_type=jnp.float32,
            )

    def inverse_of(dx):
        return lax.rsqrt(ssq_c[-dx % NX] / D + 1e-05)

    def summed(values):
        highest = jnp.max(values, axis=0, keepdims=True)
        return highest, jnp.sum(jnp.exp(values - highest), axis=0, keepdims=True)

    def lines(*rows):
        count = 2 if len(rows) == 2 else 4
        line = lax.broadcasted_iota(jnp.int32, (count, ROWS), 0)
        out = jnp.broadcast_to(rows[-1], (count, ROWS))
        for k in range(len(rows) - 2, -1, -1):
            out = jnp.where(line == k, rows[k], out)
        return out

    def code_block(dx):
        values = acc[lax.rem(x + dx, NX)] * inverse_of(dx)
        highest, total = summed(values)
        reach = jnp.maximum(highest - jnp.min(values, axis=0, keepdims=True), 1e-20)
        note_out[dx - 1] = lines(highest, total, reach)
        send(note_out.at[dx - 1], note_in.at[dx - 1], note_send.at[dx - 1], note_recv.at[dx - 1], layers[dx - 1])
        step = 2 * SPAN / reach
        code_out[dx - 1] = jnp.exp(SPAN - (highest - values) * step).astype(jnp.bfloat16)

    near_part, far_part = pl.ds(0, SPLIT), pl.ds(SPLIT, COLS - SPLIT)

    def send_block(dx):
        if dx == 2:
            send(code_out.at[1, far_part], passed, blk_send.at[3], blk_recv.at[3], at(-1, 0, 0))
            send(code_out.at[1, near_part], code_in.at[1, near_part], blk_send.at[1], blk_recv.at[1], at(2, 0, 0))
        else:
            send(code_out.at[dx - 1], code_in.at[dx - 1], blk_send.at[dx - 1], blk_recv.at[dx - 1], layers[dx - 1])

    pair_send_of(0, 0)
    rounds, x_last, plane_known, column_known = plan()
    left = {dx: 32 for dx in range(NX)}
    squares_at = {}
    to_code, to_send, ready = [], [], ()
    for r, (takes, hops) in enumerate(rounds):
        if takes and r:
            landed(held.at[pl.ds(0, len(takes)), own_half], hop_recv.at[r])
            for t in takes:
                pair_send_of(t, r)
        for way, t, lands in hops:
            shard = held.at[slot(*(a + b for a, b in zip(offset_of(t), way))), own_half]
            send(shard, shard, hop_send.at[t // 32], hop_recv.at[lands], at(*way))
        if r == squares_at.get("z"):
            exchanged(ssq_a, 0)
            ssq_b[0] = jnp.sum(ssq_a[...], axis=0)
            exchange(ssq_b, 1, column)
            squares_at["x"] = r + 5
        if r == squares_at.get("x"):
            exchanged(ssq_b, 1)
            ssq_c[0] = jnp.sum(ssq_b[...], axis=0)
            exchange(ssq_c, 2, layers)
            squares_at["done"] = r + 4
        if r == squares_at.get("done"):
            exchanged(ssq_c, 2)
        if r == 1:
            load.wait()
        if ready:
            multiply(ready, r - 1)
        for t in ready:
            left[t // 32] -= 1
            if left[t // 32] == 0 and t // 32:
                to_code.append(t // 32)
        ready = takes
        if r == plane_known:
            exchange(ssq_a, 0, plane)
            squares_at["z"] = max(r + 4, column_known)
        if r >= squares_at.get("done", 1000):
            for dx in to_code:
                code_block(dx)
                to_send.append(dx)
            to_code = []
        if r >= x_last:
            for dx in to_send:
                send_block(dx)
            to_send = []
    assert not to_code and not to_send

    mine = acc[x] * inverse_of(0)
    tops, adds = [], []
    top, add = summed(mine)
    tops.append(top)
    adds.append(add)
    for k in range(NX - 1):
        landed(note_in.at[k], note_recv.at[k])
        tops.append(note_in[k][:1])
        adds.append(note_in[k][1:2])

    def merged(tops, adds):
        top = tops[0]
        for other in tops[1:]:
            top = jnp.maximum(top, other)
        add = jnp.zeros_like(top)
        for k in range(len(tops)):
            add = add + adds[k] * jnp.exp(tops[k] - top)
        return top, add

    st_a[0] = lines(*merged(tops, adds))
    exchange(st_a, 3, plane)
    landed(passed, blk_recv.at[3])
    send(passed, code_in.at[1, far_part], blk_send.at[4], blk_recv.at[4], at(-1, 0, 0))
    puts = []

    def put(k, values):
        logits_ref[k] = values

    put(x, mine)
    exchanged(st_a, 3)
    st_b[0] = lines(*merged([st_a[k][:1] for k in range(8)], [st_a[k][1:2] for k in range(8)]))
    exchange(st_b, 4, column)

    for dx in (1, 3, 2):
        if dx == 2:
            landed(code_in.at[1, near_part], blk_recv.at[1])
            landed(code_in.at[1, far_part], blk_recv.at[4])
        else:
            landed(code_in.at[dx - 1], blk_recv.at[dx - 1])
        note = note_in[dx - 1]
        highest, reach = note[:1], note[2:3]
        step = reach / (2 * SPAN)
        values = highest - (SPAN - jnp.log(code_in[dx - 1].astype(jnp.float32))) * step
        put(lax.rem(x + NX - dx, NX), values)

    for dx in range(NX):
        landed(held.at[pl.ds(0, 32), own_half], pair_send.at[dx])
        landed(held.at[pl.ds(0, 31 if dx == 0 else 32), own_half], hop_send.at[dx])
    for k in range(NX - 1):
        landed(note_out.at[k], note_send.at[k])
        if k != 1:
            landed(code_out.at[k], blk_send.at[k])
    landed(code_out.at[1, near_part], blk_send.at[1])
    landed(passed, blk_send.at[3])
    landed(passed, blk_send.at[4])

    exchanged(st_b, 4)
    top, add = merged([st_b[k][:1] for k in range(8)], [st_b[k][1:2] for k in range(8)])
    lse_ref[...] = jnp.broadcast_to(top + jnp.log(add), (8, ROWS))
    for copy in puts:
        copy.wait()


def subtract(logits_ref, lse_ref, out_ref, out, out_sem):
    writes, begin = [], 0
    for k in range(NX):
        out[COLS * k : COLS * (k + 1), :] = logits_ref[k] - lse_ref[:1]
        end = COLS * (k + 1) if k == NX - 1 else COLS * (k + 1) // 8 * 8
        rows = pl.ds(begin, end - begin)
        writes.append(pltpu.make_async_copy(out.at[rows], out_ref.at[rows], out_sem.at[k]))
        writes[-1].start()
        begin = end
    for copy in writes:
        copy.wait()


def local(residual, gain, unembed):
    f32, bf16 = jnp.float32, jnp.bfloat16
    vmem = pl.BlockSpec(memory_space=pltpu.VMEM)
    anywhere = pl.BlockSpec(memory_space=pl.ANY)
    hbm = pl.BlockSpec(memory_space=pltpu.HBM)
    dma = pltpu.SemaphoreType.DMA
    logits, lse = pl.pallas_call(
        kernel,
        name="lens",
        out_shape=(
            jax.ShapeDtypeStruct((NX, COLS, ROWS), f32),
            jax.ShapeDtypeStruct((8, ROWS), f32),
        ),
        in_specs=[hbm, hbm, hbm],
        out_specs=(vmem, vmem),
        scratch_shapes=[
            pltpu.VMEM((ROWS, FEAT), bf16),
            pltpu.VMEM((1, FEAT), bf16),
            pltpu.VMEM((NX * NZ * NY, 2 * FEAT, ROWS), bf16),
            pltpu.VMEM((COLS, D), bf16),
            pltpu.VMEM((NX, COLS, ROWS), f32),
            pltpu.VMEM((NX - 1, COLS, ROWS), bf16),
            pltpu.VMEM((NX - 1, COLS, ROWS), bf16),
            pltpu.VMEM((COLS - SPLIT, ROWS), bf16),
            pltpu.VMEM((NX - 1, 4, ROWS), f32),
            pltpu.VMEM((NX - 1, 4, ROWS), f32),
            pltpu.VMEM((8, 1, ROWS), f32),
            pltpu.VMEM((8, 1, ROWS), f32),
            pltpu.VMEM((NX, 1, ROWS), f32),
            pltpu.VMEM((8, 2, ROWS), f32),
            pltpu.VMEM((8, 2, ROWS), f32),
            dma, dma((4,)), dma((len(plan()[0]),)), dma((4,)), dma((len(plan()[0]),)),
            dma((5,)), dma((5,)), dma((3,)), dma((3,)), dma((5,)), dma((5,)), dma((NX,)), dma((2,)),
        ],
        compiler_params=pltpu.CompilerParams(
            collective_id=0, has_side_effects=True, vmem_limit_bytes=50 * 1024 * 1024
        ),
    )(residual, gain, unembed.T)
    out = pl.pallas_call(
        subtract,
        name="subtract",
        out_shape=jax.ShapeDtypeStruct((NX * COLS, ROWS), f32),
        in_specs=[vmem, vmem],
        out_specs=anywhere,
        scratch_shapes=[pltpu.VMEM((NX * COLS, ROWS), f32), dma((NX,))],
        compiler_params=pltpu.CompilerParams(vmem_limit_bytes=8 * 1024 * 1024),
    )(logits, lse)
    return out.T


def solution(mesh):
    torus = Mesh(mesh.devices.reshape(NZ, NY, 2, mesh.shape["layer"]), AXES)
    planes = ("z", "y", "c")
    return jax.shard_map(
        local,
        mesh=torus,
        in_specs=(P("x", planes), P(None, planes), P(None, (*planes, "x"))),
        out_specs=P("x", planes),
        check_vma=False,
    )
```
